32 devices in a mesh: dp: 8 (over z, core), tp: 4 (over y, x).
Axes of the slice: x: 2, y: 2, z: 4, core: 2. Of those that a mesh axis runs over, the one named last changes fastest.
Arguments:
- hidden_states: bfloat16 [2048, 3584], P('dp'), may hold values from -21 to 21
- resp_lengths: int32 [4], replicated, may hold values from 1 to 1280, 2048 in all
- w_query: bfloat16 [3584, 512], P('dp', 'tp'), may hold values from -0.25 to 0.25
- w_keyval: bfloat16 [3584, 1024], P('dp', 'tp'), may hold values from -0.09375 to 0.09375
- w_out: bfloat16 [512, 3584], P('tp', 'dp'), may hold values from -0.25 to 0.25
Outputs:
- attended: bfloat16 [2048, 3584], P('dp', 'tp')
The draws below stay inside these ranges and needn't reach their ends.
Inputs may be any that keep to these rules, and one draw needn't show every extreme that they name: `resp_lengths`: the 4 lengths sum to 2048; the longest is exactly 1280.
All inputs are finite; a program needn't handle non-finite values.
Results may differ from the reference program's by a relative error of at most 0.015.
The reference program's roundings to bfloat16 on the way count: a program that leaves them out, or rounds other values in their place, can miss the bound.
Values may be sent and summed in bfloat16 or wider, within the bound.
No kernel may reach another device: no remote copies, remote signals or barrier semaphores. Data moves between devices by JAX's collectives and lax.ppermute only.
A program may use at most 64 MiB of HBM per device.

```python
import math
import jax
import jax.numpy as jnp
import numpy as np
from jax import lax

D = 3584
HD = 128
KV = 4
TOK_DEV = 256
HEADS = 4
TOKENS = 2048
LMAX = 1280
NRESP = 4
N_TP = 4


def draw_hidden_states(key, part):
    first_key = jax.random.fold_in(jax.random.fold_in(key, 11), 0)
    values = jnp.clip(jax.random.normal(first_key, (TOKENS, D), jnp.float32), -6.0, 6.0)
    return values.astype(jnp.bfloat16)


def level_of(stream_key, extent, shards, low, high):
    factor_of = 1.0
    for dim, parts in shards:
        draws = jax.random.uniform(jax.random.fold_in(jax.random.fold_in(stream_key, 6), dim), (parts,), jnp.float32, low / len(shards), high / len(shards))
        factor_of = factor_of * jnp.repeat(jnp.exp(draws), extent[dim] // parts).reshape((-1,) + (1,) * (len(extent) - 1 - dim))
    return factor_of


def length_profile(amount, total, reach, slope):
    portions = [(1 << 20) // math.isqrt(grade ** slope) + 1 for grade in range(2, amount + 1)]
    surplus, holding = total - reach - (amount - 1), [1] * (amount - 1)
    while surplus > 0:
        free = [i for i in range(amount - 1) if holding[i] < reach]
        whole, budget = sum([portions[i] for i in free]), surplus
        for i in free:
            extra = min(reach - holding[i], max(1, budget * portions[i] // whole), surplus)
            holding[i] = holding[i] + extra
            surplus = surplus - extra
    return np.array([reach] + holding)


def uneven_parts(own_key, amount, total, limit, skew):
    if amount == 2:
        one = jax.random.randint(own_key, (), max(1, total - limit), min(limit, total - 1) + 1)
        return jnp.stack([one, total - one])
    tallies = jnp.asarray(length_profile(amount, total, limit, skew), jnp.int32)
    couples = (amount - 1) // 2
    donor, sink = tallies[1:1 + 2 * couples:2], tallies[2:2 + 2 * couples:2]
    room = jnp.minimum(donor - 1, limit - sink)
    moved = jax.random.randint(jax.random.fold_in(own_key, 1), (couples,), 0, 1 << 20) % (room + 1)
    tallies = tallies.at[1:1 + 2 * couples:2].set(donor - moved).at[2:2 + 2 * couples:2].set(sink + moved)
    return tallies[jax.random.permutation(jax.random.fold_in(own_key, 2), amount)]


def centred(own_key, shape, width, reach, pieces=(), kind=jnp.bfloat16):
    result = width * jax.random.normal(own_key, shape, jnp.float32)
    if pieces:
        result = result * level_of(own_key, shape, pieces, -0.22, 0.18)
    return jnp.clip(result, -reach, reach).astype(kind)


def setup_inputs(seed: int = 0) -> dict:
    key_list = jax.random.split(jax.random.key(seed), 6)
    hidden_states = draw_hidden_states(jax.random.fold_in(key_list[5], 71), 0)
    resp_lengths = uneven_parts(key_list[1], NRESP, TOKENS, LMAX, 2).astype(jnp.int32)
    w_query = centred(key_list[2], (D, HEADS * HD), (D // 6) ** -0.5, 0.25, ((0, 8), (1, 4)))
    w_keyval = centred(key_list[3], (D, 2 * KV * HD), D ** -0.5, 0.09375, ((0, 8), (1, 4)))
    w_out = centred(key_list[4], (HEADS * HD, D), (HEADS * HD) ** -0.5, 0.25, ((0, 4), (1, 8)))
    return dict(hidden_states=hidden_states, resp_lengths=resp_lengths, w_query=w_query, w_keyval=w_keyval, w_out=w_out)


def reference(hidden_states, resp_lengths, w_query, w_keyval, w_out):
    total_tokens = hidden_states.shape[0]
    head_scale = HD ** -0.5
    query = (jnp.dot(hidden_states, w_query, preferred_element_type=jnp.float32) * head_scale).astype(jnp.bfloat16)
    keyval = jnp.dot(hidden_states, w_keyval, preferred_element_type=jnp.float32).astype(jnp.bfloat16)
    resp_ends = jnp.cumsum(resp_lengths, dtype=jnp.int32)
    position = jnp.arange(total_tokens, dtype=jnp.int32)
    segment = jnp.sum((position[:, None] >= resp_ends[None, :]).astype(jnp.int32), axis=1, dtype=jnp.int32)
    window = min(total_tokens, TOK_DEV + LMAX)
    blocks = total_tokens // TOK_DEV
    per_group = HEADS // KV

    def one_head(head):
        kv_head = (head // per_group).astype(jnp.int32)
        key_head = lax.dynamic_slice_in_dim(keyval, kv_head * HD, HD, 1)
        value_head = lax.dynamic_slice_in_dim(keyval, (KV + kv_head) * HD, HD, 1)
        query_head = lax.dynamic_slice_in_dim(query, (head * HD).astype(jnp.int32), HD, 1)

        def one_block(block):
            begin = (block * TOK_DEV).astype(jnp.int32)
            key_begin = jnp.clip(begin + TOK_DEV - window, 0, total_tokens - window).astype(jnp.int32)
            query_rows = lax.dynamic_slice_in_dim(query_head, begin, TOK_DEV, 0)
            key_rows = lax.dynamic_slice_in_dim(key_head, key_begin, window, 0)
            value_rows = lax.dynamic_slice_in_dim(value_head, key_begin, window, 0)
            query_pos = begin + jnp.arange(TOK_DEV, dtype=jnp.int32)
            key_pos = key_begin + jnp.arange(window, dtype=jnp.int32)
            query_seg = lax.dynamic_slice_in_dim(segment, begin, TOK_DEV, 0)
            key_seg = lax.dynamic_slice_in_dim(segment, key_begin, window, 0)
            scores = jnp.dot(query_rows, key_rows.T, preferred_element_type=jnp.float32)
            allowed = (query_seg[:, None] == key_seg[None, :]) & (key_pos[None, :] <= query_pos[:, None])
            largest = jnp.max(jnp.where(allowed, scores, jnp.float32(-1e30)), axis=1)
            expw = jnp.where(allowed, jnp.exp(scores - largest[:, None]), jnp.float32(0.0))
            denom = jnp.sum(expw, axis=1)
            numer = jnp.dot(expw.astype(jnp.bfloat16), value_rows, preferred_element_type=jnp.float32)
            return (numer / denom[:, None]).astype(jnp.bfloat16)

        return lax.map(one_block, jnp.arange(blocks, dtype=jnp.int32)).reshape(total_tokens, HD)

    heads_all = lax.map(one_head, jnp.arange(HEADS, dtype=jnp.int32))
    heads_out = jnp.transpose(heads_all, (1, 0, 2)).reshape(total_tokens, HEADS * HD)
    group_width = (HEADS // N_TP) * HD
    summed = jnp.zeros((total_tokens, w_out.shape[1]), jnp.float32)
    for group in range(N_TP):
        partial_sum = jnp.dot(heads_out[:, group * group_width:(group + 1) * group_width],
                              w_out[group * group_width:(group + 1) * group_width],
                              preferred_element_type=jnp.float32).astype(jnp.bfloat16)
        partial_sum = lax.optimization_barrier(partial_sum)
        summed = summed + partial_sum.astype(jnp.float32)
    return summed.astype(jnp.bfloat16)
```

```python
import functools

import jax
import jax.numpy as jnp
from jax import lax
from jax.experimental import pallas as pl
from jax.experimental.pallas import tpu as pltpu
from jax.sharding import PartitionSpec as P

HD = 128
CORES = 2
VMEM = pl.BlockSpec(memory_space=pltpu.VMEM)
SMEM = pl.BlockSpec(memory_space=pltpu.SMEM)


def segment_of(position, resp_ends):
    return jnp.sum(
        (position[:, None] >= resp_ends[None, :]).astype(jnp.int32), axis=1, dtype=jnp.int32
    )


def general_body(hidden_states, resp_lengths, w_query, w_keyval, w_out):
    token_rows = hidden_states.shape[0]
    head_scale = HD ** (-0.5)
    pieces = (
        lax.all_gather(w_query, "dp", axis=0, tiled=True),
        lax.all_gather(w_keyval, "dp", axis=0, tiled=True),
    )
    query_sum = jnp.dot(hidden_states, pieces[0], preferred_element_type=jnp.float32)
    keyval_sum = jnp.dot(hidden_states, pieces[1], preferred_element_type=jnp.float32)
    query = (query_sum * head_scale).astype(jnp.bfloat16)
    keyval = lax.all_gather(keyval_sum.astype(jnp.bfloat16), "tp", axis=1, tiled=True)
    kv_count = keyval.shape[1] // (2 * HD)
    per_group = lax.axis_size("tp") // kv_count
    kv_head = lax.axis_index("tp") // per_group
    key_head = lax.dynamic_slice_in_dim(keyval, kv_head * HD, HD, 1)
    value_head = lax.dynamic_slice_in_dim(keyval, (kv_count + kv_head) * HD, HD, 1)
    head_pair = jnp.concatenate([key_head, value_head], axis=1)
    resp_ends = jnp.cumsum(resp_lengths, dtype=jnp.int32)
    own_begin = lax.axis_index("dp") * token_rows
    query_pos = own_begin + jnp.arange(token_rows, dtype=jnp.int32)
    query_seg = segment_of(query_pos, resp_ends)
    pieces = lax.all_gather(head_pair, "dp", axis=0, tiled=True)
    largest = jnp.full((token_rows,), -1e30, jnp.float32)
    height = pieces.shape[0]
    key_pos = jnp.arange(height, dtype=jnp.int32)
    key_seg = segment_of(key_pos, resp_ends)
    scores = jnp.dot(query, pieces[:, :HD].T, preferred_element_type=jnp.float32)
    allowed = (
        (query_seg[:, None] == key_seg[None, :])
        & (key_pos[None, :] <= query_pos[:, None])
        & (key_pos[None, :] >= 0)
    )
    newest = jnp.maximum(largest, jnp.max(jnp.where(allowed, scores, jnp.float32(-1e30)), axis=1))
    expw = jnp.where(allowed, jnp.exp(scores - newest[:, None]), jnp.float32(0.0))
    denom = jnp.sum(expw, axis=1)
    numer = jnp.dot(expw.astype(jnp.bfloat16), pieces[:, HD:], preferred_element_type=jnp.float32)
    heads_out = (numer / denom[:, None]).astype(jnp.bfloat16)
    terms = jnp.dot(
        heads_out,
        lax.all_gather(w_out, "dp", axis=1, tiled=True),
        preferred_element_type=jnp.float32,
    )
    summed = lax.psum_scatter(terms.astype(jnp.bfloat16), "tp", scatter_dimension=1, tiled=True)
    return summed


def attend_kernel(ids_ref, lens_ref, query_ref, *refs):
    blocks, out_ref, scores_ref = refs[:-2], refs[-2], refs[-1]
    rows = query_ref.shape[0]
    query = query_ref[...]
    query_pos = ids_ref[0] * rows + lax.broadcasted_iota(jnp.int32, (rows, 1), 0)
    begin = jnp.zeros((rows, 1), jnp.int32)
    end = jnp.int32(0)
    for r in range(lens_ref.shape[0]):
        end = end + lens_ref[r]
        begin = jnp.where(query_pos >= end, end, begin)
    largest = jnp.full((rows, 1), -1e30, jnp.float32)
    for b, block in enumerate(blocks):
        scores = lax.dot_general(
            query, block[:, :HD], (((1,), (1,)), ((), ())), preferred_element_type=jnp.float32
        )
        key_pos = ids_ref[b] * rows + lax.broadcasted_iota(jnp.int32, (rows, rows), 1)
        allowed = (key_pos >= begin) & (key_pos <= query_pos)
        scores = jnp.where(allowed, scores, -1e30)
        scores_ref[:, b * rows:(b + 1) * rows] = scores
        largest = jnp.maximum(largest, jnp.max(scores, axis=1, keepdims=True))
    denom = jnp.zeros((rows, 1), jnp.float32)
    numer = jnp.zeros((rows, HD), jnp.float32)
    for b, block in enumerate(blocks):
        expw = jnp.exp(scores_ref[:, b * rows:(b + 1) * rows] - largest)
        denom = denom + jnp.sum(expw, axis=1, keepdims=True)
        numer = numer + jnp.dot(
            expw.astype(jnp.bfloat16), block[:, HD:], preferred_element_type=jnp.float32
        )
    out_ref[...] = (numer / denom).astype(jnp.bfloat16)


def attend(ids, lens, query, blocks):
    rows = query.shape[0]
    return pl.pallas_call(
        attend_kernel,
        out_shape=jax.ShapeDtypeStruct((rows, HD), jnp.bfloat16),
        in_specs=[SMEM, SMEM] + [VMEM] * (1 + len(blocks)),
        out_specs=VMEM,
        scratch_shapes=[pltpu.VMEM((rows, rows * len(blocks)), jnp.float32)],
        name="attend",
    )(ids, lens, query, *blocks)


def outward_kernel(ids_ref, weight_ref, *refs):
    heads, out_ref = refs[:-1], refs[-1]
    total = None
    for k, head in enumerate(heads):
        term = jnp.dot(head[...], weight_ref[ids_ref[k]], preferred_element_type=jnp.float32)
        term = term.astype(jnp.bfloat16).astype(jnp.float32)
        total = term if total is None else total + term
    out_ref[...] = total.astype(jnp.bfloat16)


def outward(ids, weight, heads):
    return pl.pallas_call(
        outward_kernel,
        out_shape=jax.ShapeDtypeStruct((heads[0].shape[0], weight.shape[2]), jnp.bfloat16),
        in_specs=[SMEM, VMEM] + [VMEM] * len(heads),
        out_specs=VMEM,
        name="outward",
    )(ids, weight, *heads)


def chip_body(line, tp, hidden_states, resp_lengths, w_query, w_keyval, w_out):
    def permute(value, target):
        pairs = []
        for z in range(line):
            for c in range(CORES):
                for t in range(tp):
                    z2, c2, t2 = target(z, c, t)
                    if 0 <= z2 < line:
                        pairs.append(((z * CORES + c) * tp + t, (z2 * CORES + c2) * tp + t2))
        return lax.ppermute(value, ("dp", "tp"), pairs)

    def swap(value):
        return permute(value, lambda z, c, t: (z, 1 - c, t))

    def onward(value):
        return permute(value, lambda z, c, t: (z + 1 - 2 * c, c, t))

    own = lax.axis_index("dp")
    t = lax.axis_index("tp")
    z, c = own // CORES, own % CORES
    rows = hidden_states.shape[0]

    def pair(mine, other, axis):
        return jnp.where(
            c == 0,
            jnp.concatenate([mine, other], axis),
            jnp.concatenate([other, mine], axis),
        )

    def gather(mine):
        slab = pair(mine, swap(mine), 0)
        found = [(z, slab)]
        for s in range(1, line):
            slab = onward(slab)
            found.append((z + (2 * c - 1) * s, slab))
            found.append((z - (2 * c - 1) * s, swap(slab)))
        return found

    def project(found):
        total = None
        for index, slab in found:
            depth = slab.shape[0]
            part = lax.dynamic_slice_in_dim(
                hidden_states, jnp.clip(index, 0, line - 1) * depth, depth, 1
            )
            term = jnp.dot(part, slab, preferred_element_type=jnp.float32)
            total = term if total is None else total + term
        return total

    half = tp // 2
    low = t < half
    first, second = w_keyval[:, :HD], w_keyval[:, HD:]
    sent = (jnp.where(low, first, second), jnp.where(low, second, first))
    got_a = permute(
        sent[0], lambda z, c, t: (z, c, 2 * t if t < half else 2 * (t - half) + 1)
    )
    got_b = permute(
        sent[1], lambda z, c, t: (z, c, 2 * t + 1 if t < half else 2 * (t - half))
    )
    even = t % 2 == 0
    w_head = jnp.concatenate(
        [jnp.where(even, got_a, got_b), jnp.where(even, got_b, got_a)], axis=1
    )

    query = (project(gather(w_query)) * HD ** (-0.5)).astype(jnp.bfloat16)
    keyval = project(gather(w_head)).astype(jnp.bfloat16)

    blocks = [(own, keyval), (2 * z + 1 - c, swap(keyval))]
    for k in range(1, line):
        block = permute(keyval, lambda z, c, t, k=k: (z + k, c, t))
        blocks.append((own - CORES * k, block))
        blocks.append((2 * (z - k) + 1 - c, swap(block)))
    ids = jnp.stack([index for index, _ in blocks]).astype(jnp.int32)
    heads_out = attend(ids, resp_lengths, query, [block for _, block in blocks])

    out_blocks = [
        permute(w_out, lambda z, c, t, m=m: (t ^ m, c, z)) for m in range(line)
    ]
    out_mine = jnp.stack(out_blocks)
    out_weight = pair(out_mine, swap(out_mine), 2)
    heads = [heads_out] + [
        permute(heads_out, lambda z, c, t, k=k: (z, c, t ^ k)) for k in range(1, tp)
    ]
    order = jnp.stack([t ^ z ^ k for k in range(tp)]).astype(jnp.int32)
    return outward(order, out_weight, heads)


def solution(mesh):
    dp, tp = mesh.shape["dp"], mesh.shape["tp"]
    line = dp // CORES

    def body(hidden_states, resp_lengths, w_query, w_keyval, w_out):
        by_chip = (
            dp % CORES == 0
            and line == tp
            and tp & (tp - 1) == 0
            and w_query.shape[1] == HD
            and w_keyval.shape[1] == CORES * HD
        )
        form = functools.partial(chip_body, line, tp) if by_chip else general_body
        return form(hidden_states, resp_lengths, w_query, w_keyval, w_out)

    return jax.shard_map(
        body,
        mesh=mesh,
        in_specs=(P("dp", None), P(), P("dp", "tp"), P("dp", "tp"), P("tp", "dp")),
        out_specs=P("dp", "tp"),
        check_vma=False,
    )
```

```python
import functools

import jax
import jax.numpy as jnp
from jax import lax
from jax.experimental import pallas as pl
from jax.experimental.pallas import tpu as pltpu
from jax.sharding import PartitionSpec as P

HD = 128
CORES = 2
VMEM = pl.BlockSpec(memory_space=pltpu.VMEM)
SMEM = pl.BlockSpec(memory_space=pltpu.SMEM)


def segment_of(position, resp_ends):
    return jnp.sum(
        (position[:, None] >= resp_ends[None, :]).astype(jnp.int32), axis=1, dtype=jnp.int32
    )


def general_body(hidden_states, resp_lengths, w_query, w_keyval, w_out):
    token_rows = hidden_states.shape[0]
    head_scale = HD ** (-0.5)
    pieces = (
        lax.all_gather(w_query, "dp", axis=0, tiled=True),
        lax.all_gather(w_keyval, "dp", axis=0, tiled=True),
    )
    query_sum = jnp.dot(hidden_states, pieces[0], preferred_element_type=jnp.float32)
    keyval_sum = jnp.dot(hidden_states, pieces[1], preferred_element_type=jnp.float32)
    query = (query_sum * head_scale).astype(jnp.bfloat16)
    keyval = lax.all_gather(keyval_sum.astype(jnp.bfloat16), "tp", axis=1, tiled=True)
    kv_count = keyval.shape[1] // (2 * HD)
    per_group = lax.axis_size("tp") // kv_count
    kv_head = lax.axis_index("tp") // per_group
    key_head = lax.dynamic_slice_in_dim(keyval, kv_head * HD, HD, 1)
    value_head = lax.dynamic_slice_in_dim(keyval, (kv_count + kv_head) * HD, HD, 1)
    head_pair = jnp.concatenate([key_head, value_head], axis=1)
    resp_ends = jnp.cumsum(resp_lengths, dtype=jnp.int32)
    own_begin = lax.axis_index("dp") * token_rows
    query_pos = own_begin + jnp.arange(token_rows, dtype=jnp.int32)
    query_seg = segment_of(query_pos, resp_ends)
    pieces = lax.all_gather(head_pair, "dp", axis=0, tiled=True)
    largest = jnp.full((token_rows,), -1e30, jnp.float32)
    height = pieces.shape[0]
    key_pos = jnp.arange(height, dtype=jnp.int32)
    key_seg = segment_of(key_pos, resp_ends)
    scores = jnp.dot(query, pieces[:, :HD].T, preferred_element_type=jnp.float32)
    allowed = (
        (query_seg[:, None] == key_seg[None, :])
        & (key_pos[None, :] <= query_pos[:, None])
        & (key_pos[None, :] >= 0)
    )
    newest = jnp.maximum(largest, jnp.max(jnp.where(allowed, scores, jnp.float32(-1e30)), axis=1))
    expw = jnp.where(allowed, jnp.exp(scores - newest[:, None]), jnp.float32(0.0))
    denom = jnp.sum(expw, axis=1)
    numer = jnp.dot(expw.astype(jnp.bfloat16), pieces[:, HD:], preferred_element_type=jnp.float32)
    heads_out = (numer / denom[:, None]).astype(jnp.bfloat16)
    terms = jnp.dot(
        heads_out,
        lax.all_gather(w_out, "dp", axis=1, tiled=True),
        preferred_element_type=jnp.float32,
    )
    summed = lax.psum_scatter(terms.astype(jnp.bfloat16), "tp", scatter_dimension=1, tiled=True)
    return summed


def attend_kernel(place_ref, lens_ref, query_ref, *refs):
    blocks, out_ref, scores_ref = refs[:-2], refs[-2], refs[-1]
    rows, height = query_ref.shape[0], blocks[0].shape[0]
    core = place_ref[1]
    query = query_ref[...]
    chip_begin = place_ref[0] * height
    query_pos = chip_begin + core * rows + lax.broadcasted_iota(jnp.int32, (rows, 1), 0)
    begin = jnp.zeros((rows, 1), jnp.int32)
    end = jnp.int32(0)
    for r in range(lens_ref.shape[0]):
        end = end + lens_ref[r]
        begin = jnp.where(query_pos >= end, end, begin)
    pairs = [(blocks[i], blocks[i + 1]) for i in range(0, len(blocks), 2)]
    largest = jnp.full((rows, 1), -1e30, jnp.float32)
    for k, (mine, other) in enumerate(pairs):
        key = jnp.where(core == 0, mine[...], other[...])
        scores = lax.dot_general(
            query, key, (((1,), (1,)), ((), ())), preferred_element_type=jnp.float32
        )
        key_pos = chip_begin - k * height + lax.broadcasted_iota(jnp.int32, (rows, height), 1)
        allowed = (key_pos >= begin) & (key_pos <= query_pos)
        scores = jnp.where(allowed, scores, -1e30)
        scores_ref[:, k * height:(k + 1) * height] = scores
        largest = jnp.maximum(largest, jnp.max(scores, axis=1, keepdims=True))
    denom = jnp.zeros((rows, 1), jnp.float32)
    numer = jnp.zeros((rows, HD), jnp.float32)
    for k, (mine, other) in enumerate(pairs):
        value = jnp.where(core == 0, other[...], mine[...])
        expw = jnp.exp(scores_ref[:, k * height:(k + 1) * height] - largest)
        denom = denom + jnp.sum(expw, axis=1, keepdims=True)
        numer = numer + jnp.dot(
            expw.astype(jnp.bfloat16), value, preferred_element_type=jnp.float32
        )
    out_ref[...] = (numer / denom).astype(jnp.bfloat16)


def attend(place, lens, query, blocks):
    rows, height = query.shape[0], blocks[0].shape[0]
    return pl.pallas_call(
        attend_kernel,
        out_shape=jax.ShapeDtypeStruct((rows, HD), jnp.bfloat16),
        in_specs=[SMEM, SMEM] + [VMEM] * (1 + len(blocks)),
        out_specs=VMEM,
        scratch_shapes=[pltpu.VMEM((rows, height * len(blocks) // 2), jnp.float32)],
        name="attend",
    )(place, lens, query, *blocks)


def outward_kernel(count, place_ref, *refs):
    heads, mine, other = refs[:count], refs[count:2 * count], refs[2 * count:3 * count]
    out_ref, heads_ref, weight_ref = refs[3 * count:]
    core, lane = place_ref[1], place_ref[2]
    width = mine[0].shape[0]
    for k in range(count):
        heads_ref[k] = heads[k][...]
    total = None
    for m in range(count):
        weight_ref[m, pl.ds(pl.multiple_of(core * width, 16), width)] = mine[m][...]
        weight_ref[m, pl.ds(pl.multiple_of((1 - core) * width, 16), width)] = other[m][...]
        term = lax.dot_general(
            heads_ref[lane ^ m], weight_ref[m], (((1,), (1,)), ((), ())),
            preferred_element_type=jnp.float32,
        )
        term = term.astype(jnp.bfloat16).astype(jnp.float32)
        total = term if total is None else total + term
    out_ref[...] = total.astype(jnp.bfloat16)


def outward(place, heads, mine, other):
    count, rows, width = len(heads), heads[0].shape[0], mine[0].shape[0]
    return pl.pallas_call(
        functools.partial(outward_kernel, count),
        out_shape=jax.ShapeDtypeStruct((rows, CORES * width), jnp.bfloat16),
        in_specs=[SMEM] + [VMEM] * (3 * count),
        out_specs=VMEM,
        scratch_shapes=[
            pltpu.VMEM((count, rows, HD), jnp.bfloat16),
            pltpu.VMEM((count, CORES * width, HD), jnp.bfloat16),
        ],
        name="outward",
    )(place, *heads, *mine, *other)


def chip_body(line, tp, hidden_states, resp_lengths, w_query, w_keyval, w_out):
    def permute(value, target):
        pairs = []
        for z in range(line):
            for c in range(CORES):
                for t in range(tp):
                    z2, c2, t2 = target(z, c, t)
                    if 0 <= z2 < line:
                        pairs.append(((z * CORES + c) * tp + t, (z2 * CORES + c2) * tp + t2))
        return lax.ppermute(value, ("dp", "tp"), pairs)

    def swap(value):
        return permute(value, lambda z, c, t: (z, 1 - c, t))

    def shift(value, k):
        return permute(value, lambda z, c, t: (z + k, c, t))

    own = lax.axis_index("dp")
    t = lax.axis_index("tp")
    z, c = own // CORES, own % CORES
    half = line // 2

    def reach(value):
        across = permute(value, lambda z, c, t: (z + half if z < half else z - half, c, t))
        found = [(z, value), (jnp.where(z < half, z + half, z - half), across)]
        for k in range(1, half):
            found.append((z - k, shift(value, k)))
            found.append((z + k, shift(value, -k)))
        for k in range(1, half):
            far = permute(across, lambda z, c, t, k=k: (z + k if z >= half else z - k, c, t))
            found.append((jnp.where(z < half, z + half + k, z - half - k), far))
        return found

    def project(found, tokens):
        total = [None] * len(tokens)
        for index, slab in found:
            depth = slab.shape[0]
            begin = jnp.clip(index, 0, line - 1) * depth
            for i, states in enumerate(tokens):
                part = lax.dynamic_slice_in_dim(states, begin, depth, 1)
                term = jnp.dot(part, slab, preferred_element_type=jnp.float32)
                total[i] = term if total[i] is None else total[i] + term
        return total

    hidden_other = swap(hidden_states)
    tokens = (hidden_states, hidden_other)

    first, second = w_keyval[:, :HD], w_keyval[:, HD:]

    def deal(value, flip):
        def target(z, c, t):
            column = 2 * t + (1 - c if flip else c)
            return z, column // tp, column % tp

        return permute(value, target)

    got_a = deal(jnp.where(c == 0, first, second), False)
    got_b = deal(jnp.where(c == 0, second, first), True)
    w_head = jnp.where(
        t % 2 == 0,
        jnp.concatenate([got_a, got_b], 0),
        jnp.concatenate([got_b, got_a], 0),
    )

    def spread(slab):
        blank = jnp.zeros_like(slab)
        return jnp.where(
            c == 0, jnp.concatenate([slab, blank], 0), jnp.concatenate([blank, slab], 0)
        )

    query_mine, query_other = project(
        [(index, spread(slab)) for index, slab in reach(w_query)], tokens
    )
    query = ((query_mine + swap(query_other)) * HD ** (-0.5)).astype(jnp.bfloat16)

    mine, other = [part.astype(jnp.bfloat16) for part in project(reach(w_head), tokens)]
    chip = jnp.where(
        c == 0, jnp.concatenate([mine, other], 0), jnp.concatenate([other, mine], 0)
    )
    blocks = [chip, swap(chip)]
    for k in range(1, line):
        block = shift(chip, k)
        blocks += [block, swap(block)]
    place = jnp.stack([z, c, z ^ t]).astype(jnp.int32)
    heads_out = attend(place, resp_lengths, query, blocks)

    w_turned = w_out.T
    out_mine = [permute(w_turned, lambda z, c, t, m=m: (t ^ m, c, z)) for m in range(line)]
    out_other = [swap(block) for block in out_mine]
    heads = [heads_out] + [
        permute(heads_out, lambda z, c, t, k=k: (z, c, t ^ k)) for k in range(1, tp)
    ]
    return outward(place, heads, out_mine, out_other)


def solution(mesh):
    dp, tp = mesh.shape["dp"], mesh.shape["tp"]
    line = dp // CORES

    def body(hidden_states, resp_lengths, w_query, w_keyval, w_out):
        by_chip = (
            dp % CORES == 0
            and line == tp
            and line % 2 == 0
            and tp & (tp - 1) == 0
            and w_query.shape[1] == HD
            and w_keyval.shape[1] == CORES * HD
        )
        form = functools.partial(chip_body, line, tp) if by_chip else general_body
        return form(hidden_states, resp_lengths, w_query, w_keyval, w_out)

    return jax.shard_map(
        body,
        mesh=mesh,
        in_specs=(P("dp", None), P(), P("dp", "tp"), P("dp", "tp"), P("tp", "dp")),
        out_specs=P("dp", "tp"),
        check_vma=False,
    )
```
